32 devices in a mesh: dp: 8 (over z, core), tp: 4 (over y, x).
Axes of the slice: x: 2, y: 2, z: 4, core: 2. Of those that a mesh axis runs over, the one named last changes fastest.
Arguments:
- hidden: bfloat16 [384, 4096], P('dp'), may hold values from -6 to 6
- w_qkv: bfloat16 [4096, 4608], P('dp', 'tp'), may hold values from -0.09375 to 0.09375
- w_out: bfloat16 [4096, 4096], P('tp', 'dp'), may hold values from -0.125 to 0.125
- norm_gain: float32 [4096], replicated, may hold values from 0.5 to 1.5
- kv_cache: bfloat16 [384, 2, 128, 256], P(('dp', 'tp')), may hold values from -110 to 110
- lengths: int32 [384], P(('dp', 'tp')), may hold values from 1 to 127, as said below
Outputs:
- residual_out: bfloat16 [384, 4096], P('dp', 'tp')
- scaled: bfloat16 [384, 4096], P('dp', 'tp')
- row_scale: float32 [384], P('dp')
The draws below stay inside these ranges and needn't reach their ends.
Inputs may be any that keep to these rules, and one draw needn't show every extreme that they name: `lengths`: every sequence has 1 to 127 live positions; among each device's 12 sequences one has exactly 127.
All inputs are finite; a program needn't handle non-finite values.
Results may differ from the reference program's by a relative error of at most 0.015.
Values may be sent and summed in bfloat16 or wider, within the bound.
A program may use at most 64 MiB of HBM per device.

```python
import jax
import jax.numpy as jnp
from jax import lax

D = 4096
KVH = 2
HD = 128
HEADS = 32
SEQ_DEV = 12
CTX = 128
QKV = 4608
ATT = 4096
TOTAL_SEQ = 384
N_TP = 4


def draw_kv_cache(key, part):
    shape = (TOTAL_SEQ, KVH, CTX, 2 * HD)
    key_main = jax.random.fold_in(key, 11)
    values = jnp.clip(jax.random.normal(key_main, shape, jnp.float32), -6.0, 6.0)
    return values.astype(jnp.bfloat16)


def draw_lengths(key, part):
    key_base = jax.random.fold_in(key, 21)
    key_pick = jax.random.fold_in(key, 22)
    base = jax.random.randint(key_base, (TOTAL_SEQ,), 1, CTX)
    picked = jax.random.randint(key_pick, (TOTAL_SEQ // SEQ_DEV,), 0, SEQ_DEV)
    slots = jnp.arange(TOTAL_SEQ) % SEQ_DEV
    owners = jnp.arange(TOTAL_SEQ) // SEQ_DEV
    return jnp.where(slots == picked[owners], CTX - 1, base).astype(jnp.int32)


def with_spikes(entries, stream_key, source, target, blocks, factor):
    def block_of(position):
        return (jnp.arange(entries.shape[position]) // (entries.shape[position] // blocks)).reshape((-1,) + (1,) * (entries.ndim - 1 - position))

    first = jax.random.permutation(stream_key, blocks)[block_of(target)]
    other_side = (block_of(target) + blocks // 2) % blocks
    return jnp.where((block_of(source) == first) | (block_of(source) == other_side), factor * entries, entries)


def levels(stream_key, dims, shards, smallest, high):
    level = 1.0
    for axis_at, blocks in shards:
        heights = jax.random.uniform(jax.random.fold_in(jax.random.fold_in(stream_key, 6), axis_at), (blocks,), jnp.float32, smallest / len(shards), high / len(shards))
        level = level * jnp.repeat(jnp.exp(heights), dims[axis_at] // blocks).reshape((-1,) + (1,) * (len(dims) - 1 - axis_at))
    return level


def normal_values(rng, shape, spread, bound, cuts=(), kind=jnp.bfloat16):
    gain = levels(rng, shape, cuts, -0.22, 0.18) if cuts else 1.0
    result = jax.random.normal(rng, shape, jnp.float32) * spread * gain
    return jnp.minimum(jnp.maximum(result, -bound), bound).astype(kind)


def noise_with(key, shape, scale, most, shards, heavy, kind=jnp.bfloat16):
    values = scale * jax.random.normal(key, shape, jnp.float32)
    if shards:
        values = values * levels(key, shape, shards, -0.22, 0.18)
    return jnp.clip(with_spikes(values, jax.random.fold_in(key, 3), *heavy), -most, most).astype(kind)


def setup_inputs(seed: int = 0) -> dict:
    streams_of = jax.random.split(jax.random.key(seed), 7)
    hidden = normal_values(streams_of[0], (TOTAL_SEQ, D), 1.0, 6.0, ((0, 8),))
    w_qkv = normal_values(streams_of[1], (D, QKV), D ** -0.5, 0.09375, ((0, 8), (1, 4)))
    w_out = noise_with(streams_of[2], (ATT, D), ATT ** -0.5, 0.125, ((0, 4), (1, 8)), (0, 1, 8, 2.0))
    norm_gain = jnp.clip(1.0 + 0.1 * jax.random.normal(streams_of[3], (D,), jnp.float32), 0.5, 1.5)
    kv_cache = draw_kv_cache(jax.random.fold_in(streams_of[6], 71), 0)
    lengths = draw_lengths(jax.random.fold_in(streams_of[6], 71), 0)
    return {"hidden": hidden, "w_qkv": w_qkv, "w_out": w_out, "norm_gain": norm_gain, "kv_cache": kv_cache, "lengths": lengths}


def rope(values, positions):
    half = values.shape[-1] // 2
    freqs = 1000000.0 ** (-2.0 * jnp.arange(half, dtype=jnp.float32) / values.shape[-1])
    angle = positions[..., None] * freqs
    cosine = jnp.cos(angle)
    sine = jnp.sin(angle)
    first = values[..., :half]
    second = values[..., half:]
    return jnp.concatenate([first * cosine - second * sine, second * cosine + first * sine], axis=-1)

def attend(query, key_new, value_new, cache, live):
    count = query.shape[0]
    groups = HEADS // KVH
    q_grp = query.reshape(count, KVH, groups, HD).astype(jnp.float32)
    keys = cache[..., :HD].astype(jnp.float32)
    vals = cache[..., HD:].astype(jnp.float32)
    scale = 1.0 / HD ** 0.5
    scores = jnp.einsum('nkgd,nkpd->nkgp', q_grp, keys) * scale
    own = jnp.einsum('nkgd,nkd->nkg', q_grp, key_new.astype(jnp.float32)) * scale
    valid = (jnp.arange(CTX)[None, :] < live[:, None])[:, None, None, :]
    scores = jnp.where(valid, scores, jnp.float32(-1e+30))
    top = jnp.maximum(lax.optimization_barrier(jnp.max(scores, axis=-1)), own)
    probs = jnp.where(valid, jnp.exp(scores - top[..., None]), jnp.float32(0.0))
    own_prob = jnp.exp(own - top)
    denom = lax.optimization_barrier(jnp.sum(probs, axis=-1)) + own_prob
    weights = (probs / denom[..., None]).astype(jnp.bfloat16)
    own_weight = (own_prob / denom).astype(jnp.bfloat16)
    mixed = jnp.einsum('nkgp,nkpd->nkgd', weights.astype(jnp.float32), vals)
    mixed = mixed + own_weight.astype(jnp.float32)[..., None] * value_new.astype(jnp.float32)[:, :, None, :]
    return mixed.reshape(count, ATT).astype(jnp.bfloat16)

def reference(hidden, w_qkv, w_out, norm_gain, kv_cache, lengths):
    total_rows = hidden.shape[0]
    qkv = jnp.dot(hidden, w_qkv, preferred_element_type=jnp.float32).astype(jnp.bfloat16)
    positions = lengths.astype(jnp.float32)[:, None]
    query = qkv[:, :ATT].reshape(total_rows, HEADS, HD).astype(jnp.float32)
    key_new = qkv[:, ATT:ATT + KVH * HD].reshape(total_rows, KVH, HD).astype(jnp.float32)
    value_new = qkv[:, ATT + KVH * HD:].reshape(total_rows, KVH, HD)
    query = rope(query, positions).astype(jnp.bfloat16)
    key_new = rope(key_new, positions).astype(jnp.bfloat16)
    blocks = total_rows // SEQ_DEV

    def one_block(index):
        start = (index * SEQ_DEV).astype(jnp.int32)
        q_blk = lax.dynamic_slice_in_dim(query, start, SEQ_DEV, 0)
        k_blk = lax.dynamic_slice_in_dim(key_new, start, SEQ_DEV, 0)
        v_blk = lax.dynamic_slice_in_dim(value_new, start, SEQ_DEV, 0)
        c_blk = lax.dynamic_slice_in_dim(kv_cache, start, SEQ_DEV, 0)
        l_blk = lax.dynamic_slice_in_dim(lengths, start, SEQ_DEV, 0)
        return attend(q_blk, k_blk, v_blk, c_blk, l_blk)
    attn = lax.map(one_block, jnp.arange(blocks, dtype=jnp.int32)).reshape(total_rows, ATT)
    width = ATT // N_TP
    total = jnp.zeros((total_rows, D), jnp.float32)
    for shard in range(N_TP):
        partial_term = jnp.dot(attn[:, shard * width:(shard + 1) * width], w_out[shard * width:(shard + 1) * width, :], preferred_element_type=jnp.float32)
        total = total + partial_term.astype(jnp.bfloat16).astype(jnp.float32)
    resid = hidden.astype(jnp.float32) + total
    residual_out = resid.astype(jnp.bfloat16)
    inverse = lax.rsqrt(lax.optimization_barrier(jnp.mean(resid * resid, axis=-1, keepdims=True)) + 1e-06)
    normed = resid * norm_gain[None, :] * inverse
    row_scale = (lax.optimization_barrier(jnp.max(jnp.abs(normed), axis=-1)) + 1e-06) / 448.0
    scaled = (normed / row_scale[:, None]).astype(jnp.bfloat16)
    return (residual_out, scaled, row_scale)
```

```python
import functools

import jax
import jax.numpy as jnp
from jax import lax
from jax.experimental import pallas as pl
from jax.experimental.pallas import tpu as pltpu
from jax.sharding import PartitionSpec as P


def rope(values, positions):
    half = values.shape[-1] // 2
    freqs = 1000000.0 ** (-2.0 * jnp.arange(half, dtype=jnp.float32) / values.shape[-1])
    angle = positions[..., None] * freqs
    cosine = jnp.cos(angle)
    sine = jnp.sin(angle)
    first = values[..., :half]
    second = values[..., half:]
    return jnp.concatenate(
        [first * cosine - second * sine, second * cosine + first * sine], axis=-1
    )


def shards(hidden, w_qkv, w_out, norm_gain, kv_cache, lengths):
    seq_dev = kv_cache.shape[0]
    kv_heads = kv_cache.shape[1]
    head_size = kv_cache.shape[3] // 2
    tp_count = lax.axis_size("tp")
    w_cols = lax.all_gather(w_qkv, "dp", axis=0, tiled=True)
    qkv_part = jnp.dot(hidden, w_cols, preferred_element_type=jnp.float32)
    mine = lax.all_to_all(
        qkv_part.astype(jnp.bfloat16), "tp", split_axis=0, concat_axis=1, tiled=True
    )
    att_width = w_out.shape[0] * tp_count
    heads = att_width // head_size
    groups = heads // kv_heads
    positions = lengths.astype(jnp.float32)[:, None]
    query = rope(
        mine[:, :att_width].reshape(seq_dev, heads, head_size).astype(jnp.float32), positions
    ).astype(jnp.bfloat16)
    key_new = rope(
        mine[:, att_width : att_width + kv_heads * head_size]
        .reshape(seq_dev, kv_heads, head_size)
        .astype(jnp.float32),
        positions,
    ).astype(jnp.bfloat16)
    value_new = mine[:, att_width + kv_heads * head_size :].reshape(seq_dev, kv_heads, head_size)
    q_grp = query.reshape(seq_dev, kv_heads, groups, head_size)
    keys = kv_cache[..., :head_size]
    vals = kv_cache[..., head_size:]
    scale = 1.0 / head_size**0.5
    scores = jnp.einsum("nkgd,nkpd->nkgp", q_grp, keys, preferred_element_type=jnp.float32) * scale
    own = jnp.einsum("nkgd,nkd->nkg", q_grp, key_new, preferred_element_type=jnp.float32) * scale
    valid = (jnp.arange(kv_cache.shape[2])[None, :] < lengths[:, None])[:, None, None, :]
    scores = jnp.where(valid, scores, jnp.float32(-1e30))
    top = jnp.maximum(jnp.max(scores, axis=-1), own)
    probs = jnp.where(valid, jnp.exp(scores - top[..., None]), jnp.float32(0.0))
    own_prob = jnp.exp(own - top)
    denom = jnp.sum(probs, axis=-1) + own_prob
    weights = (probs / denom[..., None]).astype(jnp.bfloat16)
    own_weight = (own_prob / denom).astype(jnp.bfloat16)
    mixed = jnp.einsum("nkgp,nkpd->nkgd", weights, vals, preferred_element_type=jnp.float32)
    mixed = (
        mixed
        + own_weight.astype(jnp.float32)[..., None] * value_new.astype(jnp.float32)[:, :, None, :]
    )
    attn = mixed.reshape(seq_dev, att_width).astype(jnp.bfloat16)
    heads_part = lax.all_to_all(attn, "tp", split_axis=1, concat_axis=0, tiled=True)
    terms = jnp.dot(
        heads_part,
        lax.all_gather(w_out, "dp", axis=1, tiled=True),
        preferred_element_type=jnp.float32,
    )
    width = terms.shape[1]
    share = width // tp_count
    offset = lax.axis_index("tp") * share
    summed = lax.psum_scatter(
        terms.astype(jnp.bfloat16), "tp", scatter_dimension=1, tiled=True
    ).astype(jnp.float32)
    hidden_mine = lax.dynamic_slice_in_dim(hidden, offset, share, 1).astype(jnp.float32)
    gain_mine = lax.dynamic_slice_in_dim(norm_gain, offset, share, 0)
    resid_mine = hidden_mine + summed
    weighted = resid_mine * gain_mine[None, :]
    squares = lax.psum(jnp.sum(resid_mine * resid_mine, axis=-1), "tp")
    peak = lax.pmax(jnp.max(jnp.abs(weighted), axis=-1), "tp")
    inverse = lax.rsqrt(squares / width + 1e-06)
    normed_mine = weighted * inverse[:, None]
    row_scale = (peak * inverse + 1e-06) / 448.0
    residual_out = resid_mine.astype(jnp.bfloat16)
    scaled = (normed_mine / row_scale[:, None]).astype(jnp.bfloat16)
    return (residual_out, scaled, row_scale)


F32 = jnp.float32
BF16 = jnp.bfloat16
MESH = pl.DeviceIdType.MESH
VMEM_LIMIT = 66_000_000


def PARTS(seqs):
    return ((0, seqs),)


def send(src, dst, send_sem, recv_sem, where):
    copy = pltpu.make_async_remote_copy(
        src_ref=src, dst_ref=dst, send_sem=send_sem, recv_sem=recv_sem,
        device_id=where, device_id_type=MESH,
    )
    copy.start()
    return copy


def pick(at, table):
    out = jnp.int32(table[0])
    for k in range(1, len(table)):
        out = jnp.where(at == k, jnp.int32(table[k]), out)
    return out


def by_distance(at, count):
    tables = [sorted(range(count), key=lambda k: (abs(k - z), -k if z < count // 2 else k)) for z in range(count)]
    return [pick(at, [tables[z][i] for z in range(count)]) for i in range(count)]


def layer(
    n_dp, n_tp, parts,
    hidden, w_qkv, w_out, gain, cache, lens,
    resid_out, scaled_out, scale_out,
    com, bats,
):
    dp = lax.axis_index("dp")
    tp = lax.axis_index("tp")
    core = lax.rem(dp, 2)
    chip = dp // 2
    partner = chip * 2 + 1 - core
    n_chip = n_dp // 2
    rows = hidden.shape[0]
    seqs = rows // n_tp
    depth = w_qkv.shape[0]
    cols = w_qkv.shape[1]
    ocols = w_out.shape[1]
    owide = resid_out.shape[1]
    kvh = cache.shape[1]
    ctx = cache.shape[2]
    hd = cache.shape[3] // 2
    heads = (w_out.shape[0] * n_tp) // hd
    groups = heads // kvh
    per = cols // hd
    per_out = w_out.shape[0] // hd
    blocks = owide // hd
    width = hidden.shape[1]
    half = hd // 2
    w1, w2, kv, hid, hid32, gmine = (com[k] for k in ("w1", "w2", "kv", "hid", "hid32", "gmine"))
    loc = com["loc"]
    order = by_distance(chip, n_chip)
    peers = [lax.rem(tp + d, n_tp) for d in range(1, n_tp)]

    load_hid = pltpu.make_async_copy(hidden, hid, loc.at[0])
    load_hid.start()
    load_w1 = pltpu.make_async_copy(w_qkv, w1.at[core], loc.at[1])
    load_w1.start()
    load_w2 = pltpu.make_async_copy(w_out, w2.at[core], loc.at[2])
    load_w2.start()
    load_kv = pltpu.make_async_copy(cache, kv, loc.at[3])
    load_kv.start()

    barrier = pltpu.get_barrier_semaphore()
    for d in range(1, n_dp):
        pl.semaphore_signal(barrier, inc=1, device_id={"dp": lax.rem(dp + d, n_dp)}, device_id_type=MESH)
    for d in range(1, n_tp):
        pl.semaphore_signal(barrier, inc=1, device_id={"tp": lax.rem(tp + d, n_tp)}, device_id_type=MESH)

    load_hid.wait()
    hid32[...] = hid[...].astype(F32)
    wide = 2 * depth
    for bat, (first, n) in zip(bats, parts):
        stage = bat["a_stage"]
        for q in range(n_tp):
            stage[q * n : (q + 1) * n, :] = hid32[q * seqs + first : q * seqs + first + n, :]
        for z in range(n_chip):
            bat["a_send"][z] = stage[:, z * wide : (z + 1) * wide].astype(BF16)
    pl.semaphore_wait(barrier, n_dp + n_tp - 2)

    pending = []

    def to(z, q):
        return (z * 2 + core, q)

    def landed(dst, sem):
        pltpu.make_async_remote_copy(
            src_ref=dst, dst_ref=dst, send_sem=sem, recv_sem=sem,
            device_id=(partner, tp), device_id_type=MESH).wait_recv()

    for bat in bats:
        for z in order[1:]:
            pending.append(send(bat["a_send"].at[z], bat["a_recv"].at[chip], bat["a_s"].at[z], bat["a_r"].at[chip], to(z, tp)))
        if bat is bats[0]:
            load_w1.wait()
            swap1 = send(w1.at[core], w1.at[core], com["w_s"].at[0], com["w_r"].at[0], (partner, tp))
            load_w2.wait()
            swap2 = send(w2.at[core], w2.at[core], com["w_s"].at[1], com["w_r"].at[1], (partner, tp))
            pending += [swap1, swap2]

    gmine[...] = gain[:, pl.ds(pl.multiple_of(tp * owide, owide), owide)]
    for bat, (first, n) in zip(bats, parts):
        row_i = lax.broadcasted_iota(jnp.int32, (n, hd), 0)
        lane_i = lax.broadcasted_iota(jnp.int32, (n, hd), 1)
        live = jnp.zeros((n, hd), jnp.int32)
        for s in range(n):
            live = jnp.where(row_i == s, lens[first + s], live)
        low = lane_i < half
        index = jnp.where(low, lane_i, lane_i - half).astype(F32)
        freqs = jnp.exp(index * F32(-2.0 * 13.815510557964274 / hd))
        angle = live.astype(F32) * freqs
        bat["cosine"][...] = jnp.cos(angle)
        bat["sine"][...] = jnp.where(low, -jnp.sin(angle), jnp.sin(angle))
        for h in range(heads):
            bat["l_rows"][pl.ds(h, n, stride=heads), :] = live.astype(F32)
        for z in range(n_chip):
            for j in range(blocks):
                block = slice((z * blocks + j) * hd, (z * blocks + j + 1) * hd)
                mine = bat["a_stage"][0:n, block]
                for q in range(1, n_tp):
                    mine = jnp.where(tp == q, bat["a_stage"][q * n : (q + 1) * n, block], mine)
                bat["hidb"][z, j * n : (j + 1) * n, :] = mine
        if bat["b_stage"].shape[1] > per * n:
            for q in range(n_tp):
                bat["b_stage"][q, per * n :, :] = jnp.zeros((bat["b_stage"].shape[1] - per * n, hd), F32)

    def project_in(b, i):
        bat, (first, n) = bats[b], parts[b]
        z = order[i]
        if i:
            landed(bat["a_recv"].at[z], bat["a_r"].at[z])
            left = bat["a_recv"][z]
        else:
            left = bat["a_send"][chip]
        bat["b_mm"][...] = jnp.dot(left, w1[...].reshape(2 * depth, cols), preferred_element_type=F32)
        for q in range(n_tp):
            for e in range(per):
                bat["b_stage"][q, e * n : (e + 1) * n, :] = bat["b_mm"][q * n : (q + 1) * n, e * hd : (e + 1) * hd]
            bat["b_send"][z, q] = bat["b_stage"][q].astype(BF16)
        for q in ([tp] if i else []) + peers:
            pending.append(send(bat["b_send"].at[z, q], bat["b_recv"].at[chip, tp], bat["b_s"].at[z, q], bat["b_r"].at[chip, tp], to(z, q)))
        if not i:
            bat["b_recv"][chip, tp] = bat["b_send"][chip, tp]

    def attend(b):
        bat, (first, n) = bats[b], parts[b]
        for i, z in enumerate(order):
            for q in ([tp] if i else []) + peers:
                landed(bat["b_recv"].at[z, q], bat["b_r"].at[z, q])
        qkv = bat["qkv"]
        for q in range(n_tp):
            total = bat["b_recv"][0, q].astype(F32)
            for z in range(1, n_chip):
                total = total + bat["b_recv"][z, q].astype(F32)
            qkv[q] = total.astype(BF16).astype(F32)
        cosine = bat["cosine"][...]
        sine = bat["sine"][...]
        q_rows, k_rows, v_rows, s_rows, a_rows = (bat[k] for k in ("q_rows", "k_rows", "v_rows", "s_rows", "a_rows"))

        def head(h):
            return qkv[h // per, (h % per) * n : (h % per + 1) * n, :]

        def turn(x):
            return (x * cosine + pltpu.roll(x, half, 1) * sine).astype(BF16).astype(F32)

        for h in range(heads):
            q_rows[pl.ds(h, n, stride=heads), :] = turn(head(h))
        for k in range(kvh):
            key_new = turn(head(heads + k))
            value_new = head(heads + kvh + k)
            for g in range(groups):
                k_rows[pl.ds(k * groups + g, n, stride=heads), :] = key_new
                v_rows[pl.ds(k * groups + g, n, stride=heads), :] = value_new
        for s in range(n):
            for k in range(kvh):
                at = (s * kvh + k) * groups
                s_rows[at : at + groups, :] = lax.dot_general(
                    q_rows[at : at + groups, :].astype(BF16), kv[first + s, k, :, :hd],
                    (((1,), (1,)), ((), ())), preferred_element_type=F32)
        factor = F32(1.0 / hd**0.5)
        pos = lax.broadcasted_iota(jnp.int32, (n * heads, ctx), 1).astype(F32)
        valid = pos < bat["l_rows"][...]
        scores = jnp.where(valid, s_rows[...] * factor, F32(-1e30))
        own = jnp.sum(q_rows[...] * k_rows[...], axis=1, keepdims=True) * factor
        top = jnp.maximum(jnp.max(scores, axis=1, keepdims=True), own)
        probs = jnp.where(valid, jnp.exp(scores - top), F32(0.0))
        own_prob = jnp.exp(own - top)
        denom = jnp.sum(probs, axis=1, keepdims=True) + own_prob
        s_rows[...] = probs / denom
        own_weight = (own_prob / denom).astype(BF16).astype(F32)
        v_rows[...] = own_weight * v_rows[...]
        for s in range(n):
            for k in range(kvh):
                at = (s * kvh + k) * groups
                a_rows[at : at + groups, :] = jnp.dot(
                    s_rows[at : at + groups, :].astype(BF16), kv[first + s, k, :, hd:],
                    preferred_element_type=F32) + v_rows[at : at + groups, :]
        for q in range(n_tp):
            for e in range(per_out):
                bat["f_stage"][q, e * n : (e + 1) * n, :] = a_rows[pl.ds(q * per_out + e, n, stride=heads), :]
            bat["f_send"][q] = bat["f_stage"][q].astype(BF16)
        for i, z in enumerate(order):
            for q in ([tp] if i else []) + peers:
                pending.append(send(bat["f_send"].at[q], bat["f_recv"].at[chip, tp], bat["f_s"].at[z, q], bat["f_r"].at[chip, tp], to(z, q)))
        bat["f_recv"][chip, tp] = bat["f_send"][tp]

    def project_out(b, i):
        bat, (first, n) = bats[b], parts[b]
        z = order[i]
        for q in ([tp] if i else []) + peers:
            landed(bat["f_recv"].at[z, q], bat["f_r"].at[z, q])
        for q in range(n_tp):
            bat["f_stage"][q] = bat["f_recv"][z, q].astype(F32)
            for e in range(per_out):
                bat["o_left"][q * n : (q + 1) * n, e * hd : (e + 1) * hd] = bat["f_stage"][q, e * n : (e + 1) * n, :]
        left = bat["o_left"][...].astype(BF16)
        for c in range(2):
            bat["o_mm"][:, c * ocols : (c + 1) * ocols] = jnp.dot(left, w2[c], preferred_element_type=F32)
        for q in range(n_tp):
            for j in range(blocks):
                bat["g_stage"][q, j * n : (j + 1) * n, :] = bat["o_mm"][q * n : (q + 1) * n, j * hd : (j + 1) * hd]
            bat["g_send"][z, q] = bat["g_stage"][q].astype(BF16)
        for q in peers:
            pending.append(send(bat["g_send"].at[z, q], bat["g_recv"].at[z, tp], bat["g_s"].at[z, q], bat["g_r"].at[z, tp], to(chip, q)))

    def add_up(b, i):
        bat = bats[b]
        z = order[i]
        total = bat["g_send"][z, tp].astype(F32)
        for q in peers:
            landed(bat["g_recv"].at[z, q], bat["g_r"].at[z, q])
            total = total + bat["g_recv"][z, q].astype(F32)
        if i:
            bat["h_send"][z] = total.astype(BF16)
            pending.append(send(bat["h_send"].at[z], bat["h_recv"].at[chip], bat["h_s"].at[z], bat["h_r"].at[chip], to(z, tp)))
        else:
            bat["h_recv"][chip] = total.astype(BF16)

    def norm(b):
        bat, (first, n) = bats[b], parts[b]
        for z in order[1:]:
            landed(bat["h_recv"].at[z], bat["h_r"].at[z])
        squares = jnp.zeros((n, hd), F32)
        peak = jnp.zeros((n, hd), F32)
        resid = bat["resid"]
        for z in range(n_chip):
            resid[z] = bat["h_recv"][z].astype(F32) + bat["hidb"][z]
            bat["j_send"][z] = resid[z].astype(BF16)
        for q in peers:
            pending.append(send(bat["j_send"].at[q], bat["j_recv"].at[tp], bat["j_s"].at[q], bat["j_r"].at[tp], to(chip, q)))
        for z in range(n_chip):
            for j in range(blocks):
                part = resid[z, j * n : (j + 1) * n, :]
                squares = squares + part * part
                at = (z * blocks + j) * hd
                peak = jnp.maximum(peak, jnp.abs(part * gain[:, at : at + hd]))
        inverse = lax.rsqrt(jnp.sum(squares, axis=1, keepdims=True) / width + F32(1e-06))
        scale = (jnp.max(peak, axis=1, keepdims=True) * inverse + F32(1e-06)) / F32(448.0)
        lane_i = lax.broadcasted_iota(jnp.int32, (n, hd), 1)
        bat["c_send"][...] = jnp.where(lane_i < half, inverse / scale, scale)
        for q in peers:
            pending.append(send(bat["c_send"], bat["c_recv"].at[tp], bat["c_s"].at[q], bat["c_r"].at[tp], to(chip, q)))
        bat["j_recv"][tp] = bat["j_send"][tp]
        bat["c_recv"][tp] = bat["c_send"][...]

    def finish_rows(b, scales):
        bat, (first, n) = bats[b], parts[b]
        for q in peers:
            landed(bat["c_recv"].at[q], bat["c_r"].at[q])
            landed(bat["j_recv"].at[q], bat["j_r"].at[q])
        row_i = lax.broadcasted_iota(jnp.int32, (n, hd), 0)
        lane_i = lax.broadcasted_iota(jnp.int32, (n, hd), 1)
        for q in range(n_tp):
            bat["resid"][q] = bat["j_recv"][q].astype(F32)
            stats = bat["c_recv"][q]
            factor = jnp.broadcast_to(stats[:, 0:1], (n, hd))
            scale = jnp.broadcast_to(stats[:, half : half + 1], (n, hd))
            spread = jnp.where(lane_i == row_i + (q * seqs + first), scale, F32(0.0))
            scales = scales + jnp.sum(spread, axis=0, keepdims=True)
            at = slice(q * seqs + first, q * seqs + first + n)
            for j in range(blocks):
                block = slice(j * hd, (j + 1) * hd)
                part = bat["resid"][q, j * n : (j + 1) * n, :]
                com["r_out"][at, block] = part
                com["x_out"][at, block] = part * gmine[:, block] * factor
        return scales

    count = len(parts)
    for b in range(count):
        for i in range(n_chip):
            if b == 0 and i == 0:
                swap1.wait_recv()
            project_in(b, i)
    load_kv.wait()
    for b in range(count):
        attend(b)
    swap2.wait_recv()
    for b in range(count):
        for i in range(n_chip):
            project_out(b, i)
            if i:
                add_up(b, i - 1)
        add_up(b, n_chip - 1)
    for b in range(count):
        norm(b)
    scales = jnp.zeros((1, hd), F32)
    for b in range(count):
        scales = finish_rows(b, scales)
    scale_out[...] = jnp.broadcast_to(scales, scale_out.shape)
    resid_out[...] = com["r_out"][...].astype(BF16)
    scaled_out[...] = com["x_out"][...].astype(BF16)
    for copy in pending:
        copy.wait_send()


def finish(resid, scaled, scale, resid_out, scaled_out, scale_out):
    resid_out[...] = resid[...]
    scaled_out[...] = scaled[...]
    scale_out[...] = scale[0:1, : scale_out.shape[1]]


def fused(n_dp, n_tp, hidden, w_qkv, w_out, norm_gain, kv_cache, lengths):
    rows, width = hidden.shape
    seqs, kvh, ctx, hd2 = kv_cache.shape
    hd = hd2 // 2
    depth, cols = w_qkv.shape
    odepth, ocols = w_out.shape
    heads = odepth * n_tp // hd
    owide = width // n_tp
    chips = n_dp // 2
    per, per_out, blocks = cols // hd, odepth // hd, owide // hd
    vm = pltpu.VMEM
    dma = pltpu.SemaphoreType.DMA
    parts = PARTS(seqs)
    com = dict(
        w1=vm((2, depth, cols), BF16), w2=vm((2, odepth, ocols), BF16), kv=vm(kv_cache.shape, BF16),
        hid=vm((rows, width), BF16), hid32=vm((rows, width), F32), gmine=vm((1, owide), F32),
        r_out=vm((rows, owide), F32), x_out=vm((rows, owide), F32),
        loc=dma((4,)), w_s=dma((2,)), w_r=dma((2,)),
    )
    bats = []
    for _, n in parts:
        pad = -(-per * n // 16) * 16
        bats.append(dict(
            a_stage=vm((n_tp * n, width), F32), a_send=vm((chips, n_tp * n, 2 * depth), BF16),
            a_recv=vm((chips, n_tp * n, 2 * depth), BF16), hidb=vm((chips, blocks * n, hd), F32),
            b_mm=vm((n_tp * n, cols), F32), b_stage=vm((n_tp, pad, hd), F32),
            b_send=vm((chips, n_tp, pad, hd), BF16), b_recv=vm((chips, n_tp, pad, hd), BF16),
            qkv=vm((n_tp, pad, hd), F32), cosine=vm((n, hd), F32), sine=vm((n, hd), F32),
            q_rows=vm((n * heads, hd), F32), k_rows=vm((n * heads, hd), F32), v_rows=vm((n * heads, hd), F32),
            l_rows=vm((n * heads, hd), F32), s_rows=vm((n * heads, ctx), F32), a_rows=vm((n * heads, hd), F32),
            f_stage=vm((n_tp, per_out * n, hd), F32), f_send=vm((n_tp, per_out * n, hd), BF16),
            f_recv=vm((chips, n_tp, per_out * n, hd), BF16),
            o_left=vm((n_tp * n, odepth), F32), o_mm=vm((n_tp * n, owide), F32),
            g_stage=vm((n_tp, blocks * n, hd), F32), g_send=vm((chips, n_tp, blocks * n, hd), BF16),
            g_recv=vm((chips, n_tp, blocks * n, hd), BF16),
            h_send=vm((chips, blocks * n, hd), BF16), h_recv=vm((chips, blocks * n, hd), BF16),
            resid=vm((chips, blocks * n, hd), F32),
            j_send=vm((chips, blocks * n, hd), BF16), j_recv=vm((n_tp, blocks * n, hd), BF16),
            c_send=vm((n, hd), F32), c_recv=vm((n_tp, n, hd), F32),
            a_s=dma((chips,)), a_r=dma((chips,)), b_s=dma((chips, n_tp)), b_r=dma((chips, n_tp)),
            f_s=dma((chips, n_tp)), f_r=dma((chips, n_tp)), g_s=dma((chips, n_tp)), g_r=dma((chips, n_tp)),
            h_s=dma((chips,)), h_r=dma((chips,)), j_s=dma((n_tp,)), j_r=dma((n_tp,)), c_s=dma((n_tp,)), c_r=dma((n_tp,)),
        ))
    anywhere = pl.BlockSpec(memory_space=pl.ANY)
    in_vmem = pl.BlockSpec(memory_space=pltpu.VMEM)
    resid, scaled, scale = pl.pallas_call(
        functools.partial(layer, n_dp, n_tp, parts),
        out_shape=(
            jax.ShapeDtypeStruct((rows, owide), BF16),
            jax.ShapeDtypeStruct((rows, owide), BF16),
            jax.ShapeDtypeStruct((8, hd), F32),
        ),
        in_specs=[anywhere, anywhere, anywhere, in_vmem, anywhere, pl.BlockSpec(memory_space=pltpu.SMEM)],
        out_specs=(in_vmem, in_vmem, in_vmem),
        scratch_shapes=[com, bats],
        compiler_params=pltpu.CompilerParams(
            collective_id=0, has_side_effects=True, vmem_limit_bytes=VMEM_LIMIT),
    )(hidden, w_qkv, w_out, norm_gain.reshape(1, width), kv_cache, lengths)
    resid, scaled, scale = pl.pallas_call(
        finish,
        out_shape=(
            jax.ShapeDtypeStruct((rows, owide), BF16),
            jax.ShapeDtypeStruct((rows, owide), BF16),
            jax.ShapeDtypeStruct((1, rows), F32),
        ),
        in_specs=[in_vmem, in_vmem, in_vmem],
        out_specs=(in_vmem, in_vmem, in_vmem),
    )(resid, scaled, scale)
    return resid, scaled, scale.reshape(rows)


def solution(mesh):
    placed = (
        P("dp", None),
        P("dp", "tp"),
        P("tp", "dp"),
        P(),
        P(("dp", "tp"), None, None, None),
        P(("dp", "tp")),
    )
    n_dp, n_tp = mesh.shape["dp"], mesh.shape["tp"]

    def body(hidden, w_qkv, w_out, norm_gain, kv_cache, lengths):
        lanes = kv_cache.shape[3] // 2
        fits = (
            n_dp % 2 == 0
            and kv_cache.shape[2] == lanes
            and w_qkv.shape[1] % lanes == 0
            and w_out.shape[0] % lanes == 0
            and w_out.shape[1] % lanes == 0
            and hidden.shape[0] <= lanes
            and hidden.shape[1] // n_tp == w_out.shape[0]
            and n_dp == 2 * n_tp
            and hidden.shape[1] == n_dp * w_out.shape[1]
            and hidden.shape[1] == n_dp * w_qkv.shape[0]
        )
        if fits:
            return fused(n_dp, n_tp, hidden, w_qkv, w_out, norm_gain, kv_cache, lengths)
        return shards(hidden, w_qkv, w_out, norm_gain, kv_cache, lengths)

    return jax.shard_map(
        body,
        mesh=mesh,
        in_specs=placed,
        out_specs=(P("dp", "tp"), P("dp", "tp"), P("dp")),
        check_vma=False,
    )
```

```python
import functools

import jax
import jax.numpy as jnp
from jax import lax
from jax.experimental import pallas as pl
from jax.experimental.pallas import tpu as pltpu
from jax.sharding import PartitionSpec as P


def rope(values, positions):
    half = values.shape[-1] // 2
    freqs = 1000000.0 ** (-2.0 * jnp.arange(half, dtype=jnp.float32) / values.shape[-1])
    angle = positions[..., None] * freqs
    cosine = jnp.cos(angle)
    sine = jnp.sin(angle)
    first = values[..., :half]
    second = values[..., half:]
    return jnp.concatenate(
        [first * cosine - second * sine, second * cosine + first * sine], axis=-1
    )


def shards(hidden, w_qkv, w_out, norm_gain, kv_cache, lengths):
    seq_dev = kv_cache.shape[0]
    kv_heads = kv_cache.shape[1]
    head_size = kv_cache.shape[3] // 2
    tp_count = lax.axis_size("tp")
    w_cols = lax.all_gather(w_qkv, "dp", axis=0, tiled=True)
    qkv_part = jnp.dot(hidden, w_cols, preferred_element_type=jnp.float32)
    mine = lax.all_to_all(
        qkv_part.astype(jnp.bfloat16), "tp", split_axis=0, concat_axis=1, tiled=True
    )
    att_width = w_out.shape[0] * tp_count
    heads = att_width // head_size
    groups = heads // kv_heads
    positions = lengths.astype(jnp.float32)[:, None]
    query = rope(
        mine[:, :att_width].reshape(seq_dev, heads, head_size).astype(jnp.float32), positions
    ).astype(jnp.bfloat16)
    key_new = rope(
        mine[:, att_width : att_width + kv_heads * head_size]
        .reshape(seq_dev, kv_heads, head_size)
        .astype(jnp.float32),
        positions,
    ).astype(jnp.bfloat16)
    value_new = mine[:, att_width + kv_heads * head_size :].reshape(seq_dev, kv_heads, head_size)
    q_grp = query.reshape(seq_dev, kv_heads, groups, head_size)
    keys = kv_cache[..., :head_size]
    vals = kv_cache[..., head_size:]
    scale = 1.0 / head_size**0.5
    scores = jnp.einsum("nkgd,nkpd->nkgp", q_grp, keys, preferred_element_type=jnp.float32) * scale
    own = jnp.einsum("nkgd,nkd->nkg", q_grp, key_new, preferred_element_type=jnp.float32) * scale
    valid = (jnp.arange(kv_cache.shape[2])[None, :] < lengths[:, None])[:, None, None, :]
    scores = jnp.where(valid, scores, jnp.float32(-1e30))
    top = jnp.maximum(jnp.max(scores, axis=-1), own)
    probs = jnp.where(valid, jnp.exp(scores - top[..., None]), jnp.float32(0.0))
    own_prob = jnp.exp(own - top)
    denom = jnp.sum(probs, axis=-1) + own_prob
    weights = (probs / denom[..., None]).astype(jnp.bfloat16)
    own_weight = (own_prob / denom).astype(jnp.bfloat16)
    mixed = jnp.einsum("nkgp,nkpd->nkgd", weights, vals, preferred_element_type=jnp.float32)
    mixed = (
        mixed
        + own_weight.astype(jnp.float32)[..., None] * value_new.astype(jnp.float32)[:, :, None, :]
    )
    attn = mixed.reshape(seq_dev, att_width).astype(jnp.bfloat16)
    heads_part = lax.all_to_all(attn, "tp", split_axis=1, concat_axis=0, tiled=True)
    terms = jnp.dot(
        heads_part,
        lax.all_gather(w_out, "dp", axis=1, tiled=True),
        preferred_element_type=jnp.float32,
    )
    width = terms.shape[1]
    share = width // tp_count
    offset = lax.axis_index("tp") * share
    summed = lax.psum_scatter(
        terms.astype(jnp.bfloat16), "tp", scatter_dimension=1, tiled=True
    ).astype(jnp.float32)
    hidden_mine = lax.dynamic_slice_in_dim(hidden, offset, share, 1).astype(jnp.float32)
    gain_mine = lax.dynamic_slice_in_dim(norm_gain, offset, share, 0)
    resid_mine = hidden_mine + summed
    weighted = resid_mine * gain_mine[None, :]
    squares = lax.psum(jnp.sum(resid_mine * resid_mine, axis=-1), "tp")
    peak = lax.pmax(jnp.max(jnp.abs(weighted), axis=-1), "tp")
    inverse = lax.rsqrt(squares / width + 1e-06)
    normed_mine = weighted * inverse[:, None]
    row_scale = (peak * inverse + 1e-06) / 448.0
    residual_out = resid_mine.astype(jnp.bfloat16)
    scaled = (normed_mine / row_scale[:, None]).astype(jnp.bfloat16)
    return (residual_out, scaled, row_scale)


F32 = jnp.float32
BF16 = jnp.bfloat16
MESH = pl.DeviceIdType.MESH
VMEM_LIMIT = 56_300_000


def PARTS(seqs):
    return ((0, seqs),)


def send(src, dst, send_sem, recv_sem, where):
    copy = pltpu.make_async_remote_copy(
        src_ref=src, dst_ref=dst, send_sem=send_sem, recv_sem=recv_sem,
        device_id=where, device_id_type=MESH,
    )
    copy.start()
    return copy


def pick(at, table):
    out = jnp.int32(table[0])
    for k in range(1, len(table)):
        out = jnp.where(at == k, jnp.int32(table[k]), out)
    return out


def chip_order(at, count):
    tables = []
    for z in range(count):
        others = sorted((k for k in range(count) if k != z), key=lambda k: (abs(k - z) == 2, abs(k - z), -k if z < count // 2 else k))
        tables.append([z] + others)
    spread = all(sum(abs(k - z) == 2 for k in range(count)) == 1 for z in range(count))
    return [pick(at, [tables[z][i] for z in range(count)]) for i in range(count)], spread


def layer(
    n_dp, n_tp, parts,
    hidden, w_qkv, w_out, gain_in, cache, lens_in,
    resid_out, scaled_out, scale_out,
    com, bats,
):
    dp = lax.axis_index("dp")
    tp = lax.axis_index("tp")
    core = lax.rem(dp, 2)
    chip = dp // 2
    partner = chip * 2 + 1 - core
    n_chip = n_dp // 2
    rows = hidden.shape[0]
    seqs = rows // n_tp
    depth = w_qkv.shape[0]
    cols = w_qkv.shape[1]
    ocols = w_out.shape[1]
    owide = resid_out.shape[1]
    kvh = cache.shape[1]
    ctx = cache.shape[2]
    hd = cache.shape[3] // 2
    heads = (w_out.shape[0] * n_tp) // hd
    groups = heads // kvh
    per = cols // hd
    per_out = w_out.shape[0] // hd
    blocks = owide // hd
    width = hidden.shape[1]
    half = hd // 2
    w1, w2, kv, hid, hid32, gain, gmine, lens = (
        com[k] for k in ("w1", "w2", "kv", "hid", "hid32", "gain", "gmine", "lens"))
    loc = com["loc"]
    order, spread = chip_order(chip, n_chip)
    direct = order[1:-1] if spread else order[1:]
    peers = [lax.rem(tp + d, n_tp) for d in range(1, n_tp)]

    load_hid = pltpu.make_async_copy(hidden, hid, loc.at[0])
    load_hid.start()
    load_w1 = pltpu.make_async_copy(w_qkv, w1.at[core], loc.at[1])
    load_w1.start()
    load_w2 = pltpu.make_async_copy(w_out, w2.at[core], loc.at[2])
    load_w2.start()
    load_kv = pltpu.make_async_copy(cache, kv, loc.at[3])
    load_kv.start()
    load_gain = pltpu.make_async_copy(gain_in, gain, loc.at[4])
    load_gain.start()
    load_lens = pltpu.make_async_copy(lens_in, lens, loc.at[5])
    load_lens.start()

    barrier = pltpu.get_barrier_semaphore()
    for d in range(1, n_dp):
        pl.semaphore_signal(barrier, inc=1, device_id={"dp": lax.rem(dp + d, n_dp)}, device_id_type=MESH)
    for d in range(1, n_tp):
        pl.semaphore_signal(barrier, inc=1, device_id={"tp": lax.rem(tp + d, n_tp)}, device_id_type=MESH)

    load_hid.wait()
    wide = 2 * depth

    def own_part(z):
        return hid.at[:, pl.ds(pl.multiple_of(z * wide, wide), wide)]

    hid32[...] = hid[...].astype(F32)
    for bat, (first, n) in zip(bats, parts):
        for z in range(n_chip):
            for j in range(blocks):
                block = slice((z * blocks + j) * hd, (z * blocks + j + 1) * hd)
                mine = hid32[first : first + n, block]
                for q in range(1, n_tp):
                    mine = jnp.where(tp == q, hid32[q * seqs + first : q * seqs + first + n, block], mine)
                bat["hidb"][z, j * n : (j + 1) * n, :] = mine
        if spread:
            bat["a2_send"][...] = bat["hidb"][order[-1]].astype(BF16)
    pl.semaphore_wait(barrier, n_dp + n_tp - 2)

    pending = []

    def to(z, q):
        return (z * 2 + core, q)

    def landed(dst, sem):
        pltpu.make_async_remote_copy(
            src_ref=dst, dst_ref=dst, send_sem=sem, recv_sem=sem,
            device_id=(partner, tp), device_id_type=MESH).wait_recv()

    for bat in bats:
        if spread:
            pending.append(send(bat["a2_send"], bat["a2_recv"].at[tp], bat["a2_s"].at[tp], bat["a2_r"].at[tp], to(order[-1], tp)))
        for z in direct:
            pending.append(send(own_part(z), bat["a_recv"].at[chip], bat["a_s"].at[z], bat["a_r"].at[chip], to(z, tp)))
    load_w1.wait()
    swap1 = send(w1.at[core], w1.at[core], com["w_s"].at[0], com["w_r"].at[0], (partner, tp))
    load_w2.wait()
    swap2 = send(w2.at[core], w2.at[core], com["w_s"].at[1], com["w_r"].at[1], (partner, tp))
    pending += [swap1, swap2]

    load_lens.wait()
    load_gain.wait()
    gmine[...] = gain[:, pl.ds(pl.multiple_of(tp * owide, owide), owide)]
    for bat, (first, n) in zip(bats, parts):
        row_i = lax.broadcasted_iota(jnp.int32, (n, hd), 0)
        lane_i = lax.broadcasted_iota(jnp.int32, (n, hd), 1)
        live = jnp.zeros((n, hd), jnp.int32)
        for s in range(n):
            live = jnp.where(row_i == s, lens[first + s], live)
        low = lane_i < half
        index = jnp.where(low, lane_i, lane_i - half).astype(F32)
        freqs = jnp.exp(index * F32(-2.0 * 13.815510557964274 / hd))
        angle = live.astype(F32) * freqs
        bat["cosine"][...] = jnp.cos(angle)
        bat["sine"][...] = jnp.where(low, -jnp.sin(angle), jnp.sin(angle))
        for h in range(heads):
            bat["l_rows"][pl.ds(h, n, stride=heads), :] = live.astype(F32)
        if bat["b_stage"].shape[1] > per * n:
            for q in range(n_tp):
                bat["b_stage"][q, per * n :, :] = jnp.zeros((bat["b_stage"].shape[1] - per * n, hd), F32)

    def spread_a(b):
        bat = bats[b]
        landed(bat["a2_recv"].at[tp], bat["a2_r"].at[tp])
        for q in peers:
            pending.append(send(bat["a2_recv"].at[tp], bat["a2_recv"].at[tp], bat["a2_s"].at[q], bat["a2_r"].at[tp], to(chip, q)))

    def project_in(b, i):
        bat, (first, n) = bats[b], parts[b]
        z = order[i]
        if not i:
            left = own_part(chip)[...]
        elif spread and i == n_chip - 1:
            for q in peers:
                landed(bat["a2_recv"].at[q], bat["a2_r"].at[q])
            for q in range(n_tp):
                bat["f_stage"][q] = bat["a2_recv"][q].astype(F32)
                for j in range(blocks):
                    bat["a_left"][q * n : (q + 1) * n, j * hd : (j + 1) * hd] = bat["f_stage"][q, j * n : (j + 1) * n, :]
            left = bat["a_left"][...].astype(BF16)
        else:
            landed(bat["a_recv"].at[z], bat["a_r"].at[z])
            left = bat["a_recv"][z]
        bat["b_mm"][...] = jnp.dot(left, w1[...].reshape(2 * depth, cols), preferred_element_type=F32)
        for q in range(n_tp):
            for e in range(per):
                bat["b_stage"][q, e * n : (e + 1) * n, :] = bat["b_mm"][q * n : (q + 1) * n, e * hd : (e + 1) * hd]
            bat["b_send"][z, q] = bat["b_stage"][q].astype(BF16)
        for q in ([tp] if i else []) + peers:
            pending.append(send(bat["b_send"].at[z, q], bat["b_recv"].at[chip, tp], bat["b_s"].at[z, q], bat["b_r"].at[chip, tp], to(z, q)))
        if not i:
            bat["b_recv"][chip, tp] = bat["b_send"][chip, tp]

    def attend(b):
        bat, (first, n) = bats[b], parts[b]
        for i, z in enumerate(order):
            for q in ([tp] if i else []) + peers:
                landed(bat["b_recv"].at[z, q], bat["b_r"].at[z, q])
        qkv = bat["qkv"]
        for q in range(n_tp):
            total = bat["b_recv"][0, q].astype(F32)
            for z in range(1, n_chip):
                total = total + bat["b_recv"][z, q].astype(F32)
            qkv[q] = total.astype(BF16).astype(F32)
        cosine = bat["cosine"][...]
        sine = bat["sine"][...]
        q_rows, k_rows, v_rows, s_rows, a_rows = (bat[k] for k in ("q_rows", "k_rows", "v_rows", "s_rows", "a_rows"))

        def head(h):
            return qkv[h // per, (h % per) * n : (h % per + 1) * n, :]

        def turn(x):
            return (x * cosine + pltpu.roll(x, half, 1) * sine).astype(BF16).astype(F32)

        for h in range(heads):
            q_rows[pl.ds(h, n, stride=heads), :] = turn(head(h))
        for k in range(kvh):
            key_new = turn(head(heads + k))
            value_new = head(heads + kvh + k)
            for g in range(groups):
                k_rows[pl.ds(k * groups + g, n, stride=heads), :] = key_new
                v_rows[pl.ds(k * groups + g, n, stride=heads), :] = value_new
        for s in range(n):
            for k in range(kvh):
                at = (s * kvh + k) * groups
                s_rows[at : at + groups, :] = lax.dot_general(
                    q_rows[at : at + groups, :].astype(BF16), kv[first + s, k, :, :hd],
                    (((1,), (1,)), ((), ())), preferred_element_type=F32)
        factor = F32(1.0 / hd**0.5)
        pos = lax.broadcasted_iota(jnp.int32, (n * heads, ctx), 1).astype(F32)
        valid = pos < bat["l_rows"][...]
        scores = jnp.where(valid, s_rows[...] * factor, F32(-1e30))
        own = jnp.sum(q_rows[...] * k_rows[...], axis=1, keepdims=True) * factor
        top = jnp.maximum(jnp.max(scores, axis=1, keepdims=True), own)
        probs = jnp.where(valid, jnp.exp(scores - top), F32(0.0))
        own_prob = jnp.exp(own - top)
        denom = jnp.sum(probs, axis=1, keepdims=True) + own_prob
        s_rows[...] = probs / denom
        own_weight = (own_prob / denom).astype(BF16).astype(F32)
        v_rows[...] = own_weight * v_rows[...]
        for s in range(n):
            for k in range(kvh):
                at = (s * kvh + k) * groups
                a_rows[at : at + groups, :] = jnp.dot(
                    s_rows[at : at + groups, :].astype(BF16), kv[first + s, k, :, hd:],
                    preferred_element_type=F32) + v_rows[at : at + groups, :]
        for q in range(n_tp):
            for e in range(per_out):
                bat["f_stage"][q, e * n : (e + 1) * n, :] = a_rows[pl.ds(q * per_out + e, n, stride=heads), :]
            bat["f_send"][q] = bat["f_stage"][q].astype(BF16)
        for i, z in enumerate(order):
            for q in ([tp] if i else []) + peers:
                pending.append(send(bat["f_send"].at[q], bat["f_recv"].at[chip, tp], bat["f_s"].at[z, q], bat["f_r"].at[chip, tp], to(z, q)))
        bat["f_recv"][chip, tp] = bat["f_send"][tp]

    def project_out(b, i):
        bat, (first, n) = bats[b], parts[b]
        z = order[i]
        for q in ([tp] if i else []) + peers:
            landed(bat["f_recv"].at[z, q], bat["f_r"].at[z, q])
        for q in range(n_tp):
            bat["f_stage"][q] = bat["f_recv"][z, q].astype(F32)
            for e in range(per_out):
                bat["o_left"][q * n : (q + 1) * n, e * hd : (e + 1) * hd] = bat["f_stage"][q, e * n : (e + 1) * n, :]
        left = bat["o_left"][...].astype(BF16)
        for c in range(2):
            bat["o_mm"][:, c * ocols : (c + 1) * ocols] = jnp.dot(left, w2[c], preferred_element_type=F32)
        for q in range(n_tp):
            for j in range(blocks):
                bat["g_stage"][q, j * n : (j + 1) * n, :] = bat["o_mm"][q * n : (q + 1) * n, j * hd : (j + 1) * hd]
            bat["g_send"][z, q] = bat["g_stage"][q].astype(BF16)
        for q in peers:
            pending.append(send(bat["g_send"].at[z, q], bat["g_recv"].at[z, tp], bat["g_s"].at[z, q], bat["g_r"].at[z, tp], to(chip, q)))

    def add_up(b, i):
        bat = bats[b]
        z = order[i]
        total = bat["g_send"][z, tp].astype(F32)
        for q in peers:
            landed(bat["g_recv"].at[z, q], bat["g_r"].at[z, q])
            total = total + bat["g_recv"][z, q].astype(F32)
        if i:
            bat["h_send"][z] = total.astype(BF16)
            pending.append(send(bat["h_send"].at[z], bat["h_recv"].at[chip], bat["h_s"].at[z], bat["h_r"].at[chip], to(z, tp)))
        else:
            bat["h_recv"][chip] = total.astype(BF16)

    def norm(b):
        bat, (first, n) = bats[b], parts[b]
        for z in order[1:]:
            landed(bat["h_recv"].at[z], bat["h_r"].at[z])
        squares = jnp.zeros((n, hd), F32)
        peak = jnp.zeros((n, hd), F32)
        resid = bat["resid"]
        for z in range(n_chip):
            resid[z] = bat["h_recv"][z].astype(F32) + bat["hidb"][z]
            bat["j_send"][z] = resid[z].astype(BF16)
        for q in peers:
            pending.append(send(bat["j_send"].at[q], bat["j_recv"].at[tp], bat["j_s"].at[q], bat["j_r"].at[tp], to(chip, q)))
        for z in range(n_chip):
            for j in range(blocks):
                part = resid[z, j * n : (j + 1) * n, :]
                squares = squares + part * part
                at = (z * blocks + j) * hd
                peak = jnp.maximum(peak, jnp.abs(part * gain[:, at : at + hd]))
        inverse = lax.rsqrt(jnp.sum(squares, axis=1, keepdims=True) / width + F32(1e-06))
        scale = (jnp.max(peak, axis=1, keepdims=True) * inverse + F32(1e-06)) / F32(448.0)
        lane_i = lax.broadcasted_iota(jnp.int32, (n, hd), 1)
        bat["c_send"][...] = jnp.where(lane_i < half, inverse / scale, scale)
        for q in peers:
            pending.append(send(bat["c_send"], bat["c_recv"].at[tp], bat["c_s"].at[q], bat["c_r"].at[tp], to(chip, q)))
        bat["j_recv"][tp] = bat["j_send"][tp]
        bat["c_recv"][tp] = bat["c_send"][...]

    def finish_rows(b, scales):
        bat, (first, n) = bats[b], parts[b]
        for q in peers:
            landed(bat["c_recv"].at[q], bat["c_r"].at[q])
            landed(bat["j_recv"].at[q], bat["j_r"].at[q])
        row_i = lax.broadcasted_iota(jnp.int32, (n, hd), 0)
        lane_i = lax.broadcasted_iota(jnp.int32, (n, hd), 1)
        for q in range(n_tp):
            bat["resid"][q] = bat["j_recv"][q].astype(F32)
            stats = bat["c_recv"][q]
            factor = jnp.broadcast_to(stats[:, 0:1], (n, hd))
            scale = jnp.broadcast_to(stats[:, half : half + 1], (n, hd))
            spread = jnp.where(lane_i == row_i + (q * seqs + first), scale, F32(0.0))
            scales = scales + jnp.sum(spread, axis=0, keepdims=True)
            at = slice(q * seqs + first, q * seqs + first + n)
            for j in range(blocks):
                block = slice(j * hd, (j + 1) * hd)
                part = bat["resid"][q, j * n : (j + 1) * n, :]
                com["r_out"][at, block] = part
                com["x_out"][at, block] = part * gmine[:, block] * factor
        return scales

    count = len(parts)
    for b in range(count):
        for i in range(n_chip):
            if b == 0 and i == 0:
                swap1.wait_recv()
            project_in(b, i)
            if spread and i == 0:
                spread_a(b)
    load_kv.wait()
    for b in range(count):
        attend(b)
    swap2.wait_recv()
    for b in range(count):
        for i in range(n_chip):
            project_out(b, i)
            if i:
                add_up(b, i - 1)
        add_up(b, n_chip - 1)
    for b in range(count):
        norm(b)
    scales = jnp.zeros((1, hd), F32)
    for b in range(count):
        scales = finish_rows(b, scales)
    scale_out[...] = jnp.broadcast_to(scales, scale_out.shape)
    resid_out[...] = com["r_out"][...].astype(BF16)
    scaled_out[...] = com["x_out"][...].astype(BF16)
    for copy in pending:
        copy.wait_send()


def finish(resid, scaled, scale, resid_out, scaled_out, scale_out):
    resid_out[...] = resid[...]
    scaled_out[...] = scaled[...]
    scale_out[...] = scale[0:1, : scale_out.shape[1]]


def fused(n_dp, n_tp, hidden, w_qkv, w_out, norm_gain, kv_cache, lengths):
    rows, width = hidden.shape
    seqs, kvh, ctx, hd2 = kv_cache.shape
    hd = hd2 // 2
    depth, cols = w_qkv.shape
    odepth, ocols = w_out.shape
    heads = odepth * n_tp // hd
    owide = width // n_tp
    chips = n_dp // 2
    per, per_out, blocks = cols // hd, odepth // hd, owide // hd
    vm = pltpu.VMEM
    dma = pltpu.SemaphoreType.DMA
    parts = PARTS(seqs)
    com = dict(
        w1=vm((2, depth, cols), BF16), w2=vm((2, odepth, ocols), BF16), kv=vm(kv_cache.shape, BF16),
        hid=vm((rows, width), BF16), hid32=vm((rows, width), F32), gain=vm((1, width), F32), gmine=vm((1, owide), F32),
        lens=pltpu.SMEM((seqs,), jnp.int32),
        r_out=vm((rows, owide), F32), x_out=vm((rows, owide), F32),
        loc=dma((6,)), w_s=dma((2,)), w_r=dma((2,)),
    )
    bats = []
    for _, n in parts:
        pad = -(-per * n // 16) * 16
        bats.append(dict(
            a2_send=vm((blocks * n, hd), BF16), a2_recv=vm((n_tp, blocks * n, hd), BF16),
            a_left=vm((n_tp * n, 2 * depth), F32), a2_s=dma((n_tp,)), a2_r=dma((n_tp,)),
            a_recv=vm((chips, n_tp * n, 2 * depth), BF16), hidb=vm((chips, blocks * n, hd), F32),
            b_mm=vm((n_tp * n, cols), F32), b_stage=vm((n_tp, pad, hd), F32),
            b_send=vm((chips, n_tp, pad, hd), BF16), b_recv=vm((chips, n_tp, pad, hd), BF16),
            qkv=vm((n_tp, pad, hd), F32), cosine=vm((n, hd), F32), sine=vm((n, hd), F32),
            q_rows=vm((n * heads, hd), F32), k_rows=vm((n * heads, hd), F32), v_rows=vm((n * heads, hd), F32),
            l_rows=vm((n * heads, hd), F32), s_rows=vm((n * heads, ctx), F32), a_rows=vm((n * heads, hd), F32),
            f_stage=vm((n_tp, per_out * n, hd), F32), f_send=vm((n_tp, per_out * n, hd), BF16),
            f_recv=vm((chips, n_tp, per_out * n, hd), BF16),
            o_left=vm((n_tp * n, odepth), F32), o_mm=vm((n_tp * n, owide), F32),
            g_stage=vm((n_tp, blocks * n, hd), F32), g_send=vm((chips, n_tp, blocks * n, hd), BF16),
            g_recv=vm((chips, n_tp, blocks * n, hd), BF16),
            h_send=vm((chips, blocks * n, hd), BF16), h_recv=vm((chips, blocks * n, hd), BF16),
            resid=vm((chips, blocks * n, hd), F32),
            j_send=vm((chips, blocks * n, hd), BF16), j_recv=vm((n_tp, blocks * n, hd), BF16),
            c_send=vm((n, hd), F32), c_recv=vm((n_tp, n, hd), F32),
            a_s=dma((chips,)), a_r=dma((chips,)), b_s=dma((chips, n_tp)), b_r=dma((chips, n_tp)),
            f_s=dma((chips, n_tp)), f_r=dma((chips, n_tp)), g_s=dma((chips, n_tp)), g_r=dma((chips, n_tp)),
            h_s=dma((chips,)), h_r=dma((chips,)), j_s=dma((n_tp,)), j_r=dma((n_tp,)), c_s=dma((n_tp,)), c_r=dma((n_tp,)),
        ))
    in_hbm = pl.BlockSpec(memory_space=pltpu.HBM)
    in_vmem = pl.BlockSpec(memory_space=pltpu.VMEM)
    resid, scaled, scale = pl.pallas_call(
        functools.partial(layer, n_dp, n_tp, parts),
        out_shape=(
            jax.ShapeDtypeStruct((rows, owide), BF16),
            jax.ShapeDtypeStruct((rows, owide), BF16),
            jax.ShapeDtypeStruct((8, hd), F32),
        ),
        in_specs=[in_hbm] * 6,
        out_specs=(in_vmem, in_vmem, in_vmem),
        scratch_shapes=[com, bats],
        compiler_params=pltpu.CompilerParams(
            collective_id=0, has_side_effects=True, vmem_limit_bytes=VMEM_LIMIT),
    )(hidden, w_qkv, w_out, norm_gain.reshape(1, width), kv_cache, lengths)
    resid, scaled, scale = pl.pallas_call(
        finish,
        out_shape=(
            jax.ShapeDtypeStruct((rows, owide), BF16),
            jax.ShapeDtypeStruct((rows, owide), BF16),
            jax.ShapeDtypeStruct((1, rows), F32),
        ),
        in_specs=[in_vmem, in_vmem, in_vmem],
        out_specs=(in_vmem, in_vmem, in_vmem),
        compiler_params=pltpu.CompilerParams(vmem_limit_bytes=2_000_000),
    )(resid, scaled, scale)
    return resid, scaled, scale.reshape(rows)


def solution(mesh):
    placed = (
        P("dp", None),
        P("dp", "tp"),
        P("tp", "dp"),
        P(),
        P(("dp", "tp"), None, None, None),
        P(("dp", "tp")),
    )
    n_dp, n_tp = mesh.shape["dp"], mesh.shape["tp"]

    def body(hidden, w_qkv, w_out, norm_gain, kv_cache, lengths):
        lanes = kv_cache.shape[3] // 2
        fits = (
            n_dp % 2 == 0
            and kv_cache.shape[2] == lanes
            and w_qkv.shape[1] % lanes == 0
            and w_out.shape[0] % lanes == 0
            and w_out.shape[1] % lanes == 0
            and hidden.shape[0] <= lanes
            and hidden.shape[1] // n_tp == w_out.shape[0]
            and n_dp == 2 * n_tp
            and hidden.shape[1] == n_dp * w_out.shape[1]
            and hidden.shape[1] == n_dp * w_qkv.shape[0]
        )
        if fits:
            return fused(n_dp, n_tp, hidden, w_qkv, w_out, norm_gain, kv_cache, lengths)
        return shards(hidden, w_qkv, w_out, norm_gain, kv_cache, lengths)

    return jax.shard_map(
        body,
        mesh=mesh,
        in_specs=placed,
        out_specs=(P("dp", "tp"), P("dp", "tp"), P("dp")),
        check_vma=False,
    )
```
